32 devices in a mesh: owner: 8 (over z, core), sub: 4 (over y, x).
Axes of the slice: x: 2, y: 2, z: 4, core: 2. Of those that a mesh axis runs over, the one named last changes fastest.
Arguments:
- residual: float32 [256, 4608], P('owner', 'sub'), may hold values from -6 to 6
- counts: int32 [8, 16], P('owner', 'sub'), may hold values from 1 to 36
- assembly: int32 [8, 16, 36, 2304], P('owner', 'sub'), may hold values from 0 to 1, as said below
- level_two: float32 [8, 2304, 2304], P('owner', 'sub'), as said below
- block_inverse: float32 [8, 2304, 144], P('owner', 'sub'), as said below
Outputs:
- corrections: float32 [256, 4608], P('owner', 'sub')
- level_residual: float32 [8, 2304, 256], P('owner', 'sub')
The draws below stay inside these ranges and needn't reach their ends.
Inputs may be any that keep to these rules, and one draw needn't show every extreme that they name: `assembly`: every row of each [36, 2304] block holds exactly one 1; split the 2304 columns into 4 equal ranges and a group's positions into runs of 4: the 144 rows of one run (live or not) put at most 72 of their 1s into one range, and in every run some range gets exactly 72. `level_two`: each group's matrix is symmetric positive definite. `block_inverse`: each diagonal block is symmetric positive definite.
All inputs are finite; a program needn't handle non-finite values.
Results may differ from the reference program's by a relative error of at most 0.0003.
Values sent between devices are 32-bit elements; how exact they have to be, the bound alone decides.
A program may use at most 64 MiB of HBM per device.

```python
import math
import jax
import jax.numpy as jnp
from jax import lax

PRIM = 36
NC = 2304
BLOCK = 144
ITERS = 4
SUB_DEV = 4
RHS = 256
GSUBS = 16
GROUPS = 8
SUBS = 128
ROUTE = 72
N_OWNER = 8
N_SUB = 4


def one_run(key):
    rows = SUB_DEV * PRIM
    held = NC // N_SUB
    key_a, key_b, key_c, key_d = jax.random.split(key, 4)
    first = jax.random.randint(key_a, (), 0, N_SUB).astype(jnp.int32)
    others = jax.random.permutation(key_b, (N_SUB - 1) * ROUTE).astype(jnp.int32)
    other_holder = others // ROUTE
    other_holder = other_holder + (other_holder >= first).astype(jnp.int32)
    holders = jnp.concatenate([jnp.zeros((ROUTE,), jnp.int32) + first, other_holder[:rows - ROUTE]])
    holders = jax.random.permutation(key_c, holders)
    offsets = jax.random.randint(key_d, (rows,), 0, held).astype(jnp.int32)
    return holders * held + offsets


def draw_assembly(key, part):
    keys = jax.random.split(jax.random.fold_in(key, 11), GROUPS * N_SUB)
    picks = jax.vmap(one_run)(keys).reshape(GROUPS, GSUBS, PRIM)
    columns = lax.broadcasted_iota(jnp.int32, (GROUPS, GSUBS, PRIM, NC), 3)
    return (columns == picks[..., None]).astype(jnp.int32)


def one_matrix(key):
    key_a, key_b, key_c = jax.random.split(key, 3)
    noise = jax.random.normal(key_a, (NC, NC), jnp.float32)
    eye = jnp.eye(NC, dtype=jnp.float32)
    off = (noise + noise.T) * (0.5 / math.sqrt(NC)) * (1.0 - eye)
    rowsum = jnp.sum(jnp.abs(off), axis=1)
    lift = jax.random.uniform(key_b, (NC,), jnp.float32, 0.05, 1.0) * jnp.mean(rowsum)
    diag = 1.25 * rowsum + lift
    matrix = (off + diag[:, None] * eye) / jnp.mean(diag)
    return matrix


def draw_level_two(key, part):
    keys = jax.random.split(jax.random.fold_in(key, 23), GROUPS)
    return lax.map(one_matrix, keys)


def draw_block_inverse(key, part):
    nblocks = NC // BLOCK
    key_a, key_b = jax.random.split(jax.random.fold_in(key, 37))
    noise = jax.random.uniform(key_a, (GROUPS, nblocks, BLOCK, BLOCK), jnp.float32, -1.0, 1.0)
    eye = jnp.eye(BLOCK, dtype=jnp.float32)
    off = (noise + jnp.swapaxes(noise, 2, 3)) * (0.2 / BLOCK) * (1.0 - eye)
    diag = jnp.exp(jax.random.uniform(key_b, (GROUPS, nblocks, BLOCK), jnp.float32, -0.7, 0.7))
    blocks = off + diag[..., None] * eye
    return blocks.reshape(GROUPS, NC, BLOCK)


def with_ends(values, key, low, largest):
    extent = values.shape
    spot = [jax.random.randint(jax.random.fold_in(key, axis), (), 0, extent[axis]) for axis in range(len(extent))]
    values = values.at[tuple(spot)].set(low)
    longest = extent.index(max(extent))
    spot[longest] = (spot[longest] + 1) % extent[longest]
    return values.at[tuple(spot)].set(largest)


def block_scale(own_key, extent, cuts, smallest, largest):
    gain, own = 1.0, jax.random.fold_in(own_key, 6)
    for position, shards_of in cuts:
        steps = jnp.exp(jax.random.uniform(jax.random.fold_in(own, position), (shards_of,), jnp.float32, smallest / len(cuts), largest / len(cuts)))
        gain = gain * jnp.repeat(steps, extent[position] // shards_of).reshape([-1 if axis == position else 1 for axis in range(len(extent))])
    return gain


def gaussian(own_key, shape, width, most, shards=(), kind=jnp.bfloat16):
    array = width * jax.random.normal(own_key, shape, jnp.float32)
    if shards:
        array = array * block_scale(own_key, shape, shards, -0.22, 0.18)
    return jnp.clip(array, -most, most).astype(kind)


def setup_inputs(seed: int = 0) -> dict:
    key_list = jax.random.split(jax.random.key(seed), 6)
    return {
        "residual": gaussian(key_list[0], (RHS, SUBS * PRIM), 1.0, 6.0, ((0, 8), (1, 4)), jnp.float32),
        "counts": with_ends(jax.random.randint(key_list[1], (GROUPS, GSUBS), 1, PRIM + 1), jax.random.fold_in(key_list[1], 1), 1, PRIM).astype(jnp.int32),
        "assembly": draw_assembly(jax.random.fold_in(key_list[5], 71), 0),
        "level_two": draw_level_two(jax.random.fold_in(key_list[5], 71), 0),
        "block_inverse": draw_block_inverse(jax.random.fold_in(key_list[5], 71), 0),
    }


def precondition(inverse, vector):
    nblocks = NC // BLOCK
    blocks = inverse.reshape(nblocks, BLOCK, BLOCK)
    shaped = vector.reshape(nblocks, BLOCK, RHS)
    return jnp.einsum("bij,bjr->bir", blocks, shaped, precision=lax.Precision.HIGHEST).reshape(NC, RHS)


def solve_group(items):
    local, count_row, blocks, matrix, inverse = items
    live = (lax.broadcasted_iota(jnp.int32, (GSUBS, PRIM), 1) < count_row[:, None]).astype(jnp.float32)
    basis = blocks.reshape(GSUBS * PRIM, NC).astype(jnp.float32) * live.reshape(GSUBS * PRIM)[:, None]
    rhs = jnp.dot(basis.T, local, precision=lax.Precision.HIGHEST, preferred_element_type=jnp.float32)
    solution = jnp.zeros((NC, RHS), jnp.float32)
    resid = rhs
    zvec = precondition(inverse, resid)
    direction = zvec
    rz_now = jnp.sum(resid * zvec, axis=0)
    for step in range(ITERS):
        image = jnp.dot(matrix, direction, precision=lax.Precision.HIGHEST, preferred_element_type=jnp.float32)
        alpha = rz_now / jnp.sum(direction * image, axis=0)
        solution = solution + alpha * direction
        resid = resid - alpha * image
        zvec = precondition(inverse, resid)
        rz_next = jnp.sum(resid * zvec, axis=0)
        direction = zvec + (rz_next / rz_now) * direction
        rz_now = rz_next
    corr = jnp.dot(basis, solution, precision=lax.Precision.HIGHEST, preferred_element_type=jnp.float32)
    return corr, resid


def reference(residual, counts, assembly, level_two, block_inverse):
    shaped = residual.reshape(RHS, N_SUB, N_OWNER, SUB_DEV, PRIM)
    local = jnp.transpose(shaped, (2, 1, 3, 4, 0)).reshape(N_OWNER, GSUBS * PRIM, RHS)
    corr, resid = lax.map(solve_group, (local, counts, assembly, level_two, block_inverse))
    back = corr.reshape(N_OWNER, N_SUB, SUB_DEV, PRIM, RHS)
    corrections = jnp.transpose(back, (4, 1, 0, 2, 3)).reshape(RHS, SUBS * PRIM)
    return corrections, resid
```

```python
import functools

import jax
import jax.numpy as jnp
from jax import lax
from jax.experimental import pallas as pl
from jax.experimental.pallas import tpu as pltpu
from jax.sharding import PartitionSpec as P

ITERS = 4
LANES = 128
MESH = pl.DeviceIdType.MESH
F32 = jnp.float32
BF16 = jnp.bfloat16


def split(value):
    high = value.astype(BF16)
    return high, (value - high.astype(F32)).astype(BF16)


def split_cat(value):
    return jnp.concatenate(split(value), axis=1)


def fold(value):
    return value[:, :LANES] + value[:, LANES:]


def rows8(value):
    return jnp.sum(value.reshape(value.shape[0] // 8, 8, value.shape[1]), axis=0)


def dot(left, right):
    return jnp.dot(left, right, preferred_element_type=F32)


def total(acc):
    return jnp.sum(acc, axis=0, keepdims=True)


def kernel(
    dims,
    res_ref,
    trow_ref,
    tcol_ref,
    binv_ref,
    corner_ref,
    mat_hbm,
    corr_out,
    resid_out,
    mat,
    mat_hi,
    mat_lo,
    pcat,
    pvec,
    xvec,
    rvec,
    zvec,
    wbuf,
    wlast,
    inv_buf,
    cor_buf,
    inv_hi,
    inv_lo,
    tbuf,
    send_pieces,
    recv_pieces,
    lbuf,
    lcat,
    xcat,
    pick,
    pw_buf,
    corr_pieces,
    corr_back,
    mat_sem,
    sub_send,
    sub_recv,
    small_send,
    small_recv,
    own_send,
    own_recv,
):
    no, ns, rows, width, block, local, rhs = dims
    chunks = rhs // LANES
    nblk = width // block
    per = rows // block
    tail = block - LANES
    quota = rhs // no
    mo = lax.axis_index("owner")
    me = lax.axis_index("sub")
    relay = ns == 4
    pending = []

    def at(ref, start, size):
        return ref.at[pl.ds(pl.multiple_of(start, 8), size)]

    def remote(src, dst, ssem, rsem, where):
        return pltpu.make_async_remote_copy(
            src_ref=src, dst_ref=dst, send_sem=ssem, recv_sem=rsem, device_id=where,
            device_id_type=MESH,
        )

    mat_copy = pltpu.make_async_copy(mat_hbm.at[0], mat, mat_sem)
    mat_copy.start()

    barrier = pltpu.get_barrier_semaphore()
    for step in range(1, ns):
        pl.semaphore_signal(
            barrier, inc=1, device_id={"sub": lax.rem(me + step, ns)}, device_id_type=MESH
        )
    for step in range(1, no):
        pl.semaphore_signal(
            barrier, inc=1, device_id={"owner": lax.rem(mo + step, no)}, device_id_type=MESH
        )

    piece = local
    for part in range(no):
        send_pieces[part * quota : (part + 1) * quota, :] = res_ref[
            :, part * piece : (part + 1) * piece
        ]
    pl.semaphore_wait(barrier, ns - 1 + no - 1)

    class Gather:
        def __init__(self, index, buf, size, src=None):
            self.index, self.buf, self.size, self.src = index, buf, size, src
            self.copies = []

        def own(self, start, size):
            if self.src is not None:
                return self.src.at[pl.ds(start, size)]
            return at(self.buf, me * self.size + start, size)

        def add(self, kind, src, dst, peer):
            copy = remote(
                src, dst, sub_send.at[self.index, kind], sub_recv.at[self.index, kind],
                {"sub": peer},
            )
            copy.start()
            self.copies.append(copy)
            pending.append(copy)

        def start(self):
            size = self.size
            if relay:
                half = size // 2
                xn = me + 1 - 2 * lax.rem(me, 2)
                yn = lax.rem(me + 2, ns)
                self.xn, self.yn, self.half = xn, yn, half
                for kind, (peer, part) in enumerate(((xn, 0), (yn, 1), (xn, 1), (yn, 0))):
                    self.add(
                        kind, self.own(part * half, half),
                        at(self.buf, me * size + part * half, half), peer,
                    )
            else:
                for step in range(1, ns):
                    self.add(
                        step - 1, self.own(0, size), at(self.buf, me * size, size),
                        lax.rem(me + step, ns),
                    )

        def forward(self):
            if relay:
                size, half = self.size, self.half
                self.copies[0].wait_recv()
                first = at(self.buf, self.xn * size, half)
                self.add(4, first, first, self.yn)
                self.copies[1].wait_recv()
                second = at(self.buf, self.yn * size + half, half)
                self.add(5, second, second, self.xn)

        def finish(self):
            for copy in self.copies[2:] if relay else self.copies:
                copy.wait_recv()

    def small_gather(index, buf, size):
        copies = []
        for step in range(1, ns):
            mine = at(buf, me * size, size)
            copy = remote(
                mine, mine, small_send.at[index, step - 1], small_recv.at[index, step - 1],
                {"sub": lax.rem(me + step, ns)},
            )
            copy.start()
            copies.append(copy)
            pending.append(copy)
        return copies

    def exchange(index, src, dst):
        copies = []
        for step in range(1, no):
            peer = lax.rem(mo + step, no)
            copy = remote(
                at(src, peer * quota, quota), at(dst, mo * quota, quota),
                own_send.at[index, step - 1], own_recv.at[index, step - 1], {"owner": peer},
            )
            copy.start()
            copies.append(copy)
            pending.append(copy)
        mine = pl.ds(pl.multiple_of(mo * quota, 8), quota)
        dst[mine, :] = src[mine, :]
        return copies

    routed = exchange(0, send_pieces, recv_pieces)
    tbuf[pl.ds(pl.multiple_of(me * 8, 8), 8), :] = trow_ref[...]
    targets = small_gather(0, tbuf, 8)
    inv_gather = Gather(0, inv_buf, rows, binv_ref)
    inv_gather.start()
    cor_buf[pl.ds(pl.multiple_of(me * per * tail, 8), per * tail), :] = corner_ref[...]
    corners = small_gather(1, cor_buf, per * tail)
    inv_buf[pl.ds(pl.multiple_of(me * rows, 8), rows), :] = binv_ref[...]

    for copy in routed:
        copy.wait_recv()
    for c in range(chunks):
        lbuf[pl.ds(pl.multiple_of(me * local, 8), local), c * LANES : (c + 1) * LANES] = (
            recv_pieces[c * LANES : (c + 1) * LANES, :].T
        )
    local_gather = Gather(1, lbuf, local)
    local_gather.start()

    mat_copy.wait()
    strip = 48

    @pl.loop(0, rows // strip)
    def _(t):
        here = pl.ds(pl.multiple_of(t * strip, strip), strip)
        high, low = split(mat[here, :])
        mat_hi[here, :] = high
        mat_lo[here, :] = low

    for lane in range(0, width, 2 * LANES):
        spot = lax.broadcasted_iota(jnp.int32, (local, 2 * LANES), 1).astype(F32) + float(lane)
        pick[:, lane : lane + 2 * LANES] = jnp.where(spot == tcol_ref[...], 1.0, 0.0).astype(BF16)

    inv_gather.forward()
    local_gather.forward()
    for copy in corners:
        copy.wait_recv()
    inv_gather.finish()

    @pl.loop(0, nblk)
    def _(b):
        rows_b = inv_buf[pl.ds(pl.multiple_of(b * block, block), block), :]
        corner = cor_buf[pl.ds(pl.multiple_of(b * tail, tail), tail), :][:, :tail]
        right = jnp.concatenate([rows_b[LANES:, :].T, corner], axis=0)
        full = jnp.concatenate([rows_b, right], axis=1)
        high, low = split(full)
        inv_hi[b] = high
        inv_lo[b] = low

    for copy in targets:
        copy.wait_recv()
    local_gather.finish()

    @pl.loop(0, ns)
    def _(s):
        here = pl.ds(pl.multiple_of(s * local, local), local)
        for c in range(chunks):
            lcat[here, 2 * c * LANES : 2 * (c + 1) * LANES] = split_cat(
                lbuf[here, c * LANES : (c + 1) * LANES]
            )

    @pl.loop(0, nblk)
    def _(b):
        here = pl.ds(pl.multiple_of(b * block, block), block)
        spot = (lax.broadcasted_iota(jnp.int32, (block, local), 0) + b * block).astype(F32)
        acc = jnp.zeros((block, 2 * rhs), F32)
        for s in range(ns):
            hot = jnp.where(spot == tbuf[s * 8 : s * 8 + 1, :], 1.0, 0.0).astype(BF16)
            acc += dot(hot, lcat[s * local : (s + 1) * local, :])
        for c in range(chunks):
            rvec[c, here, :] = fold(acc[:, 2 * c * LANES : 2 * (c + 1) * LANES])

    group = 4 if nblk % 4 == 0 else 1

    def over_blocks(body):
        def step(t, acc):
            for u in range(group):
                b = t * group + u
                acc = acc + body(b, pl.ds(pl.multiple_of(b * block, block), block))
            return acc

        return lax.fori_loop(0, nblk // group, step, jnp.zeros((8, LANES), F32))

    def precond(b, resid):
        rcat = split_cat(resid)
        return fold(dot(inv_hi[b], rcat) + dot(inv_lo[b], rcat))

    tile = 2 * block if rows % (2 * block) == 0 else block

    def matvec(c, store):
        @pl.loop(0, rows // tile)
        def _(t):
            here = pl.ds(pl.multiple_of(t * tile, tile), tile)
            store(
                t * tile,
                fold(dot(mat_hi[here, :], pcat[c]) + dot(mat_lo[here, :], pcat[c])),
            )

    def send_image(step, c):
        def store(start, value):
            wbuf[step, c, pl.ds(pl.multiple_of(me * rows + start, 8), tile), :] = value

        matvec(c, store)
        gather = Gather(2 + step * chunks + c, wbuf.at[step, c], rows)
        gather.start()
        return gather

    def first(c):
        def body(b, here):
            resid = rvec[c, here, :]
            z = precond(b, resid)
            pvec[c, here, :] = z
            xvec[c, here, :] = jnp.zeros((block, LANES), F32)
            pcat[c, here, :] = split_cat(z)
            return rows8(resid * z)

        return total(over_blocks(body))

    def update(step, c, rz):
        pw = total(over_blocks(lambda b, here: rows8(pvec[c, here, :] * wbuf[step, c, here, :])))
        alpha = rz / pw

        def body(b, here):
            resid = rvec[c, here, :] - alpha * wbuf[step, c, here, :]
            rvec[c, here, :] = resid
            xvec[c, here, :] = xvec[c, here, :] + alpha * pvec[c, here, :]
            z = precond(b, resid)
            zvec[here, :] = z
            return rows8(resid * z)

        rz_next = total(over_blocks(body))
        beta = rz_next / rz

        @pl.loop(0, nblk)
        def _(b):
            here = pl.ds(pl.multiple_of(b * block, block), block)
            p = zvec[here, :] + beta * pvec[c, here, :]
            pvec[c, here, :] = p
            pcat[c, here, :] = split_cat(p)

        return rz_next

    rz, flight = [], []
    for c in range(chunks):
        rz.append(first(c))
        flight.append(send_image(0, c))

    sums = []
    for step in range(ITERS - 1):
        for c in range(chunks):
            flight[c].forward()
        for c in range(chunks):
            flight[c].finish()
            rz[c] = update(step, c, rz[c])
            if step < ITERS - 2:
                flight[c] = send_image(step + 1, c)
            else:

                def store(start, value, c=c):
                    wlast[c, pl.ds(pl.multiple_of(start, 8), tile), :] = value

                matvec(c, store)

                def partial(t, acc, c=c):
                    here = pl.ds(pl.multiple_of(t * block, block), block)
                    there = pl.ds(pl.multiple_of(me * rows + t * block, 8), block)
                    return acc + rows8(pvec[c, there, :] * wlast[c, here, :])

                pw_buf[c, pl.ds(pl.multiple_of(me * 8, 8), 8), :] = lax.fori_loop(
                    0, per, partial, jnp.zeros((8, LANES), F32)
                )
                sums.append(small_gather(2 + c, pw_buf.at[c], 8))

    for c in range(chunks):

        @pl.loop(0, nblk)
        def _(b, c=c):
            here = pl.ds(pl.multiple_of(b * block, block), block)
            xcat[here, :] = split_cat(xvec[c, here, :])

        base = fold(dot(pick[...], xcat[...]))
        slope = fold(dot(pick[...], pcat[c]))
        for copy in sums[c]:
            copy.wait_recv()
        alpha = rz[c] / total(rows8(pw_buf[c]))
        corr_pieces[c * LANES : (c + 1) * LANES, :] = (base + alpha * slope).T
        resid_out[0, :, c * LANES : (c + 1) * LANES] = (
            rvec[c, pl.ds(pl.multiple_of(me * rows, 8), rows), :] - alpha * wlast[c]
        )
    back = exchange(1, corr_pieces, corr_back)
    for copy in back:
        copy.wait_recv()
    for part in range(no):
        corr_out[:, part * piece : (part + 1) * piece] = corr_back[
            part * quota : (part + 1) * quota, :
        ]
    for copy in pending:
        copy.wait_send()


def shards(no, ns, residual, counts, assembly, level_two, block_inverse):
    _, slots, prim, width = assembly.shape
    rows = level_two.shape[1]
    block = block_inverse.shape[2]
    local = slots * prim
    quota = residual.shape[0]
    rhs = quota * no
    chunks = rhs // LANES
    nblk = width // block
    per = rows // block
    tail = block - LANES
    live = lax.broadcasted_iota(jnp.int32, (slots, prim), 1) < counts[0][:, None]
    flat = assembly[0]
    spot = jnp.sum(flat * lax.broadcasted_iota(jnp.int32, flat.shape, 2), axis=2)
    target = jnp.where(live, spot, -1).astype(F32).reshape(local)
    trow = jnp.broadcast_to(target[None, :], (8, local))
    tcol = target[:, None]
    inverse = block_inverse[0]
    corner = inverse.reshape(per, block, block)[:, LANES:, LANES:].reshape(per * tail, tail)
    corner = jnp.pad(corner, ((0, 0), (0, LANES - tail)))
    kinds = 6 if ns == 4 else ns - 1
    vmem = pl.BlockSpec(memory_space=pltpu.VMEM)
    dma = pltpu.SemaphoreType.DMA
    dims = (no, ns, rows, width, block, local, rhs)
    return pl.pallas_call(
        functools.partial(kernel, dims),
        out_shape=(
            jax.ShapeDtypeStruct(residual.shape, F32),
            jax.ShapeDtypeStruct((1, rows, rhs), F32),
        ),
        in_specs=[vmem] * 5 + [pl.BlockSpec(memory_space=pl.ANY)],
        out_specs=(vmem, vmem),
        scratch_shapes=[
            pltpu.VMEM((rows, width), F32),
            pltpu.VMEM((rows, width), BF16),
            pltpu.VMEM((rows, width), BF16),
            pltpu.VMEM((chunks, width, 2 * LANES), BF16),
            pltpu.VMEM((chunks, width, LANES), F32),
            pltpu.VMEM((chunks, width, LANES), F32),
            pltpu.VMEM((chunks, width, LANES), F32),
            pltpu.VMEM((width, LANES), F32),
            pltpu.VMEM((ITERS - 1, chunks, width, LANES), F32),
            pltpu.VMEM((chunks, rows, LANES), F32),
            pltpu.VMEM((width, LANES), F32),
            pltpu.VMEM((nblk * tail, LANES), F32),
            pltpu.VMEM((nblk, block, block), BF16),
            pltpu.VMEM((nblk, block, block), BF16),
            pltpu.VMEM((ns * 8, local), F32),
            pltpu.VMEM((rhs, local), F32),
            pltpu.VMEM((rhs, local), F32),
            pltpu.VMEM((ns * local, rhs), F32),
            pltpu.VMEM((ns * local, 2 * rhs), BF16),
            pltpu.VMEM((width, 2 * LANES), BF16),
            pltpu.VMEM((local, width), BF16),
            pltpu.VMEM((chunks, ns * 8, LANES), F32),
            pltpu.VMEM((rhs, local), F32),
            pltpu.VMEM((rhs, local), F32),
            dma,
            dma((2 + (ITERS - 1) * chunks, kinds)),
            dma((2 + (ITERS - 1) * chunks, kinds)),
            dma((2 + chunks, ns - 1)),
            dma((2 + chunks, ns - 1)),
            dma((2, no - 1)),
            dma((2, no - 1)),
        ],
        compiler_params=pltpu.CompilerParams(
            collective_id=0, has_side_effects=True, vmem_limit_bytes=60 * 1024 * 1024
        ),
    )(residual, trow, tcol, inverse[:, :LANES], corner, level_two)


def solution(mesh):
    in_specs = (
        P("owner", "sub"),
        P("owner", "sub"),
        P("owner", "sub", None, None),
        P("owner", "sub", None),
        P("owner", "sub", None),
    )
    out_specs = (P("owner", "sub"), P("owner", "sub", None))
    body = functools.partial(shards, mesh.shape["owner"], mesh.shape["sub"])
    return jax.shard_map(body, mesh=mesh, in_specs=in_specs, out_specs=out_specs, check_vma=False)
```

```python
import functools

import jax
import jax.numpy as jnp
from jax import lax
from jax.experimental import pallas as pl
from jax.experimental.pallas import tpu as pltpu
from jax.sharding import PartitionSpec as P

ITERS = 4
LANES = 128
MESH = pl.DeviceIdType.MESH
F32 = jnp.float32
BF16 = jnp.bfloat16


def split(value):
    high = value.astype(BF16)
    return high, (value - high.astype(F32)).astype(BF16)


def split_cat(value):
    return jnp.concatenate(split(value), axis=1)


def fold(value):
    return value[:, :LANES] + value[:, LANES:]


def rows8(value):
    return jnp.sum(value.reshape(value.shape[0] // 8, 8, value.shape[1]), axis=0)


def dot(left, right):
    return jnp.dot(left, right, preferred_element_type=F32)


def total(acc):
    return jnp.sum(acc, axis=0, keepdims=True)


def kernel(
    dims,
    res_ref,
    counts_ref,
    hot_hbm,
    inv_hbm,
    mat_hbm,
    corr_out,
    resid_out,
    mat,
    mat_hi,
    mat_lo,
    pcat,
    pvec,
    xvec,
    rvec,
    zvec,
    wbuf,
    wlast,
    inv_buf,
    cor_buf,
    inv_hi,
    inv_lo,
    tbuf,
    send_pieces,
    recv_pieces,
    lbuf,
    lcat,
    xcat,
    pick,
    pw_buf,
    corr_pieces,
    corr_back,
    inv_own,
    hot_own,
    tcol,
    mat_sem,
    inv_sem,
    hot_sem,
    sub_send,
    sub_recv,
    small_send,
    small_recv,
    own_send,
    own_recv,
):
    no, ns, rows, width, block, local, rhs = dims
    chunks = rhs // LANES
    nblk = width // block
    per = rows // block
    tail = block - LANES
    quota = rhs // no
    mo = lax.axis_index("owner")
    me = lax.axis_index("sub")
    relay = ns == 4
    pending = []

    def at(ref, start, size):
        return ref.at[pl.ds(pl.multiple_of(start, 8), size)]

    def remote(src, dst, ssem, rsem, where):
        return pltpu.make_async_remote_copy(
            src_ref=src, dst_ref=dst, send_sem=ssem, recv_sem=rsem, device_id=where,
            device_id_type=MESH,
        )

    mat_copy = pltpu.make_async_copy(mat_hbm.at[0], mat, mat_sem)
    inv_copies = [
        pltpu.make_async_copy(
            inv_hbm.at[0, :, pl.ds(0, LANES)], at(inv_buf, me * rows, rows), inv_sem.at[0]
        ),
        pltpu.make_async_copy(inv_hbm.at[0], inv_own, inv_sem.at[1]),
    ]
    hot_copy = pltpu.make_async_copy(hot_hbm.at[0], hot_own, hot_sem)
    for copy in inv_copies:
        copy.start()
    hot_copy.start()
    mat_copy.start()

    barrier = pltpu.get_barrier_semaphore()
    for step in range(1, ns):
        pl.semaphore_signal(
            barrier, inc=1, device_id={"sub": lax.rem(me + step, ns)}, device_id_type=MESH
        )
    for step in range(1, no):
        pl.semaphore_signal(
            barrier, inc=1, device_id={"owner": lax.rem(mo + step, no)}, device_id_type=MESH
        )

    piece = local
    for part in range(no):
        send_pieces[part * quota : (part + 1) * quota, :] = res_ref[
            :, part * piece : (part + 1) * piece
        ]
    pl.semaphore_wait(barrier, ns - 1 + no - 1)

    class Gather:
        def __init__(self, index, buf, size, src=None):
            self.index, self.buf, self.size, self.src = index, buf, size, src
            self.copies = []

        def own(self, start, size):
            if self.src is not None:
                return self.src.at[pl.ds(start, size)]
            return at(self.buf, me * self.size + start, size)

        def add(self, kind, src, dst, peer):
            copy = remote(
                src, dst, sub_send.at[self.index, kind], sub_recv.at[self.index, kind],
                {"sub": peer},
            )
            copy.start()
            self.copies.append(copy)
            pending.append(copy)

        def start(self):
            size = self.size
            if relay:
                half = size // 2
                xn = me + 1 - 2 * lax.rem(me, 2)
                yn = lax.rem(me + 2, ns)
                self.xn, self.yn, self.half = xn, yn, half
                for kind, (peer, part) in enumerate(((xn, 0), (yn, 1), (xn, 1), (yn, 0))):
                    self.add(
                        kind, self.own(part * half, half),
                        at(self.buf, me * size + part * half, half), peer,
                    )
            else:
                for step in range(1, ns):
                    self.add(
                        step - 1, self.own(0, size), at(self.buf, me * size, size),
                        lax.rem(me + step, ns),
                    )

        def forward(self):
            if relay:
                size, half = self.size, self.half
                self.copies[0].wait_recv()
                first = at(self.buf, self.xn * size, half)
                self.add(4, first, first, self.yn)
                self.copies[1].wait_recv()
                second = at(self.buf, self.yn * size + half, half)
                self.add(5, second, second, self.xn)

        def finish(self):
            for copy in self.copies[2:] if relay else self.copies:
                copy.wait_recv()

    def small_gather(index, buf, size):
        copies = []
        for step in range(1, ns):
            mine = at(buf, me * size, size)
            copy = remote(
                mine, mine, small_send.at[index, step - 1], small_recv.at[index, step - 1],
                {"sub": lax.rem(me + step, ns)},
            )
            copy.start()
            copies.append(copy)
            pending.append(copy)
        return copies

    def exchange(index, src, dst):
        copies = []
        for step in range(1, no):
            peer = lax.rem(mo + step, no)
            copy = remote(
                at(src, peer * quota, quota), at(dst, mo * quota, quota),
                own_send.at[index, step - 1], own_recv.at[index, step - 1], {"owner": peer},
            )
            copy.start()
            copies.append(copy)
            pending.append(copy)
        mine = pl.ds(pl.multiple_of(mo * quota, 8), quota)
        dst[mine, :] = src[mine, :]
        return copies

    routed = exchange(0, send_pieces, recv_pieces)
    inv_copies[0].wait()
    inv_gather = Gather(0, inv_buf, rows)
    inv_gather.start()
    inv_copies[1].wait()
    for q in range(per):
        corner_own = inv_own[q * block + LANES : (q + 1) * block, :][:, LANES:]
        cor_buf[pl.ds(pl.multiple_of((me * per + q) * tail, 8), tail), :] = jnp.concatenate(
            [corner_own, jnp.zeros((tail, LANES - tail), F32)], axis=1
        )
    corners = small_gather(1, cor_buf, per * tail)

    hot_copy.wait()
    slots, prim = hot_own.shape[0], hot_own.shape[1]
    for q in range(slots):
        acc = jnp.zeros((prim, LANES), F32)
        spot = lax.broadcasted_iota(jnp.int32, (prim, LANES), 1)
        for lane in range(0, width, LANES):
            acc += (hot_own[q, :, lane : lane + LANES] * (spot + lane)).astype(F32)
        value = jnp.sum(acc, axis=1, keepdims=True)
        alive = lax.broadcasted_iota(jnp.int32, (prim, 1), 0) < counts_ref[0, q]
        tcol[q * prim : (q + 1) * prim, :] = jnp.broadcast_to(
            jnp.where(alive, value, -1.0), (prim, LANES)
        )
    tbuf[pl.ds(pl.multiple_of(me * 8, 8), 8), :] = tcol[...].T[:8, :]
    targets = small_gather(0, tbuf, 8)

    for copy in routed:
        copy.wait_recv()
    for c in range(chunks):
        lbuf[pl.ds(pl.multiple_of(me * local, 8), local), c * LANES : (c + 1) * LANES] = (
            recv_pieces[c * LANES : (c + 1) * LANES, :].T
        )
    local_gather = Gather(1, lbuf, local)
    local_gather.start()

    mat_copy.wait()
    strip = 48

    @pl.loop(0, rows // strip)
    def _(t):
        here = pl.ds(pl.multiple_of(t * strip, strip), strip)
        high, low = split(mat[here, :])
        mat_hi[here, :] = high
        mat_lo[here, :] = low

    for lane in range(0, width, 2 * LANES):
        spot = lax.broadcasted_iota(jnp.int32, (local, 2 * LANES), 1).astype(F32) + float(lane)
        pick[:, lane : lane + 2 * LANES] = jnp.where(spot == tcol[:, :1], 1.0, 0.0).astype(BF16)

    inv_gather.forward()
    local_gather.forward()
    for copy in corners:
        copy.wait_recv()
    inv_gather.finish()

    @pl.loop(0, nblk)
    def _(b):
        rows_b = inv_buf[pl.ds(pl.multiple_of(b * block, block), block), :]
        corner = cor_buf[pl.ds(pl.multiple_of(b * tail, tail), tail), :][:, :tail]
        right = jnp.concatenate([rows_b[LANES:, :].T, corner], axis=0)
        full = jnp.concatenate([rows_b, right], axis=1)
        high, low = split(full)
        inv_hi[b] = high
        inv_lo[b] = low

    for copy in targets:
        copy.wait_recv()
    local_gather.finish()

    @pl.loop(0, ns)
    def _(s):
        here = pl.ds(pl.multiple_of(s * local, local), local)
        for c in range(chunks):
            lcat[here, 2 * c * LANES : 2 * (c + 1) * LANES] = split_cat(
                lbuf[here, c * LANES : (c + 1) * LANES]
            )

    @pl.loop(0, nblk)
    def _(b):
        here = pl.ds(pl.multiple_of(b * block, block), block)
        spot = (lax.broadcasted_iota(jnp.int32, (block, local), 0) + b * block).astype(F32)
        acc = jnp.zeros((block, 2 * rhs), F32)
        for s in range(ns):
            hot = jnp.where(spot == tbuf[s * 8 : s * 8 + 1, :], 1.0, 0.0).astype(BF16)
            acc += dot(hot, lcat[s * local : (s + 1) * local, :])
        for c in range(chunks):
            rvec[c, here, :] = fold(acc[:, 2 * c * LANES : 2 * (c + 1) * LANES])

    group = 4 if nblk % 4 == 0 else 1

    def over_blocks(body):
        def step(t, acc):
            for u in range(group):
                b = t * group + u
                acc = acc + body(b, pl.ds(pl.multiple_of(b * block, block), block))
            return acc

        return lax.fori_loop(0, nblk // group, step, jnp.zeros((8, LANES), F32))

    def precond(b, resid):
        rcat = split_cat(resid)
        return fold(dot(inv_hi[b], rcat) + dot(inv_lo[b], rcat))

    tile = 2 * block if rows % (2 * block) == 0 else block

    def matvec(c, store):
        @pl.loop(0, rows // tile)
        def _(t):
            here = pl.ds(pl.multiple_of(t * tile, tile), tile)
            store(
                t * tile,
                fold(dot(mat_hi[here, :], pcat[c]) + dot(mat_lo[here, :], pcat[c])),
            )

    def send_image(step, c, earlier):
        def store(start, value):
            wbuf[step, c, pl.ds(pl.multiple_of(me * rows + start, 8), tile), :] = value

        matvec(c, store)
        if earlier is not None:
            earlier.forward()
        gather = Gather(2 + step * chunks + c, wbuf.at[step, c], rows)
        gather.start()
        return gather

    def first(c):
        def body(b, here):
            resid = rvec[c, here, :]
            z = precond(b, resid)
            pvec[c, here, :] = z
            xvec[c, here, :] = jnp.zeros((block, LANES), F32)
            pcat[c, here, :] = split_cat(z)
            return rows8(resid * z)

        return total(over_blocks(body))

    def update(step, c, rz):
        pw = total(over_blocks(lambda b, here: rows8(pvec[c, here, :] * wbuf[step, c, here, :])))
        alpha = rz / pw

        def body(b, here):
            resid = rvec[c, here, :] - alpha * wbuf[step, c, here, :]
            rvec[c, here, :] = resid
            xvec[c, here, :] = xvec[c, here, :] + alpha * pvec[c, here, :]
            z = precond(b, resid)
            zvec[here, :] = z
            return rows8(resid * z)

        rz_next = total(over_blocks(body))
        beta = rz_next / rz

        @pl.loop(0, nblk)
        def _(b):
            here = pl.ds(pl.multiple_of(b * block, block), block)
            p = zvec[here, :] + beta * pvec[c, here, :]
            pvec[c, here, :] = p
            pcat[c, here, :] = split_cat(p)

        return rz_next

    rz, flight, earlier = [], [], None
    for c in range(chunks):
        rz.append(first(c))
        earlier = send_image(0, c, earlier)
        flight.append(earlier)

    for step in range(ITERS - 2):
        for c in range(chunks):
            flight[c].finish()
            rz[c] = update(step, c, rz[c])
            earlier = send_image(step + 1, c, earlier)
            flight[c] = earlier

    def conclude(c, sums, base, slope):
        for copy in sums:
            copy.wait_recv()
        alpha = rz[c] / total(rows8(pw_buf[c]))
        corr_pieces[c * LANES : (c + 1) * LANES, :] = (base + alpha * slope).T
        resid_out[0, :, c * LANES : (c + 1) * LANES] = (
            rvec[c, pl.ds(pl.multiple_of(me * rows, 8), rows), :] - alpha * wlast[c]
        )

    for c in range(chunks):
        if c == chunks - 1 and chunks == 1:
            earlier.forward()
        flight[c].finish()
        rz[c] = update(ITERS - 2, c, rz[c])
        if c == chunks - 2:
            earlier.forward()

        def store(start, value, c=c):
            wlast[c, pl.ds(pl.multiple_of(start, 8), tile), :] = value

        matvec(c, store)

        def partial(t, acc, c=c):
            here = pl.ds(pl.multiple_of(t * block, block), block)
            there = pl.ds(pl.multiple_of(me * rows + t * block, 8), block)
            return acc + rows8(pvec[c, there, :] * wlast[c, here, :])

        pw_buf[c, pl.ds(pl.multiple_of(me * 8, 8), 8), :] = lax.fori_loop(
            0, per, partial, jnp.zeros((8, LANES), F32)
        )
        sums = small_gather(2 + c, pw_buf.at[c], 8)

        @pl.loop(0, nblk)
        def _(b, c=c):
            here = pl.ds(pl.multiple_of(b * block, block), block)
            xcat[here, :] = split_cat(xvec[c, here, :])

        base = fold(dot(pick[...], xcat[...]))
        slope = fold(dot(pick[...], pcat[c]))
        conclude(c, sums, base, slope)
    back = exchange(1, corr_pieces, corr_back)
    for copy in back:
        copy.wait_recv()
    for part in range(no):
        corr_out[:, part * piece : (part + 1) * piece] = corr_back[
            part * quota : (part + 1) * quota, :
        ]
    for copy in pending:
        copy.wait_send()


def shards(no, ns, residual, counts, assembly, level_two, block_inverse):
    _, slots, prim, width = assembly.shape
    rows = level_two.shape[1]
    block = block_inverse.shape[2]
    local = slots * prim
    quota = residual.shape[0]
    rhs = quota * no
    chunks = rhs // LANES
    nblk = width // block
    per = rows // block
    tail = block - LANES
    kinds = 6 if ns == 4 else ns - 1
    vmem = pl.BlockSpec(memory_space=pltpu.VMEM)
    dma = pltpu.SemaphoreType.DMA
    dims = (no, ns, rows, width, block, local, rhs)
    return pl.pallas_call(
        functools.partial(kernel, dims),
        out_shape=(
            jax.ShapeDtypeStruct(residual.shape, F32),
            jax.ShapeDtypeStruct((1, rows, rhs), F32),
        ),
        in_specs=[vmem, pl.BlockSpec(memory_space=pltpu.SMEM)]
        + [pl.BlockSpec(memory_space=pl.ANY)] * 3,
        out_specs=(vmem, vmem),
        scratch_shapes=[
            pltpu.VMEM((rows, width), F32),
            pltpu.VMEM((rows, width), BF16),
            pltpu.VMEM((rows, width), BF16),
            pltpu.VMEM((chunks, width, 2 * LANES), BF16),
            pltpu.VMEM((chunks, width, LANES), F32),
            pltpu.VMEM((chunks, width, LANES), F32),
            pltpu.VMEM((chunks, width, LANES), F32),
            pltpu.VMEM((width, LANES), F32),
            pltpu.VMEM((ITERS - 1, chunks, width, LANES), F32),
            pltpu.VMEM((chunks, rows, LANES), F32),
            pltpu.VMEM((width, LANES), F32),
            pltpu.VMEM((nblk * tail, LANES), F32),
            pltpu.VMEM((nblk, block, block), BF16),
            pltpu.VMEM((nblk, block, block), BF16),
            pltpu.VMEM((ns * 8, local), F32),
            pltpu.VMEM((rhs, local), F32),
            pltpu.VMEM((rhs, local), F32),
            pltpu.VMEM((ns * local, rhs), F32),
            pltpu.VMEM((ns * local, 2 * rhs), BF16),
            pltpu.VMEM((width, 2 * LANES), BF16),
            pltpu.VMEM((local, width), BF16),
            pltpu.VMEM((chunks, ns * 8, LANES), F32),
            pltpu.VMEM((rhs, local), F32),
            pltpu.VMEM((rhs, local), F32),
            pltpu.VMEM((rows, block), F32),
            pltpu.VMEM((slots, prim, width), jnp.int32),
            pltpu.VMEM((local, LANES), F32),
            dma,
            dma((2,)),
            dma,
            dma((2 + (ITERS - 1) * chunks, kinds)),
            dma((2 + (ITERS - 1) * chunks, kinds)),
            dma((2 + chunks, ns - 1)),
            dma((2 + chunks, ns - 1)),
            dma((2, no - 1)),
            dma((2, no - 1)),
        ],
        compiler_params=pltpu.CompilerParams(
            collective_id=0, has_side_effects=True, vmem_limit_bytes=60 * 1024 * 1024
        ),
    )(residual, counts, assembly, block_inverse, level_two)


def solution(mesh):
    in_specs = (
        P("owner", "sub"),
        P("owner", "sub"),
        P("owner", "sub", None, None),
        P("owner", "sub", None),
        P("owner", "sub", None),
    )
    out_specs = (P("owner", "sub"), P("owner", "sub", None))
    body = functools.partial(shards, mesh.shape["owner"], mesh.shape["sub"])
    return jax.shard_map(body, mesh=mesh, in_specs=in_specs, out_specs=out_specs, check_vma=False)
```
